32 devices in a mesh: dp: 32 (over z, y, x, core), feat: 1.
Axes of the slice: x: 2, y: 2, z: 4, core: 2. Of those that a mesh axis runs over, the one named last changes fastest.
Arguments:
- grads: bfloat16 [16384, 4096], P('dp', 'feat'), may hold values from -6 to 6
- covariance: float32 [4096, 4096], P('dp', 'feat'), may hold values from -0.16 to 6, as said below
- test_grads: bfloat16 [512, 4096], P('feat', 'dp'), may hold values from -0.09375 to 0.09375
- inverse_factor: bfloat16 [4096, 4096], P('dp'), may hold values from -0.09375 to 0.09375
Outputs:
- scores: float32 [16384, 512], P('dp', 'feat')
- covariance_out: float32 [4096, 4096], P('dp', 'feat')
The draws below stay inside these ranges and needn't reach their ends.
Inputs may be any that keep to these rules, and one draw needn't show every extreme that they name: covariance is symmetric.
All inputs are finite; a program needn't handle non-finite values.
Results may differ from the reference program's by a relative error of at most 0.0029.
Values may be sent and summed in bfloat16 or wider, within the bound.
A program may use at most 256 MiB of HBM per device.

```python
import jax
import jax.numpy as jnp

K = 4096
M = 512
TOKENS = 16384


def draw_covariance(key, part):
    base_key = jax.random.fold_in(key, 11)
    noise_key, diag_key = jax.random.split(base_key, 2)
    noise = jnp.clip(jax.random.normal(noise_key, (K, K), jnp.float32) * 0.007, -0.04, 0.04)
    symmetric = (noise + noise.T) * 0.5
    identity_mat = jnp.eye(K, dtype=jnp.float32)
    diagonal = jax.random.uniform(diag_key, (K,), jnp.float32, 0.5, 1.5)
    result = symmetric * (1.0 - identity_mat) + identity_mat * diagonal[None, :]
    return result


def strengthened(drawn, own_key, source, target, blocks, factor):
    owner, partner = [(jnp.arange(drawn.shape[dim]) // (drawn.shape[dim] // blocks)).reshape([-1 if axis == dim else 1 for axis in range(drawn.ndim)]) for dim in (source, target)]
    chosen = jax.random.permutation(own_key, blocks)[partner]
    strong = (owner == chosen) | (owner == (partner + blocks // 2) % blocks)
    return jnp.where(strong, factor * drawn, drawn)


def shard_levels(key, dims, shards, low, largest):
    gain = 1.0
    for dim, parts in shards:
        steps = jax.random.uniform(jax.random.fold_in(jax.random.fold_in(key, 6), dim), (parts,), jnp.float32, low / len(shards), largest / len(shards))
        gain = gain * jnp.repeat(jnp.exp(steps), dims[dim] // parts).reshape((-1,) + (1,) * (len(dims) - 1 - dim))
    return gain


def scatter_about(own_key, dims, deviation, bound, shards=(), kind=jnp.bfloat16):
    values = deviation * jax.random.normal(own_key, dims, jnp.float32)
    if shards:
        values = values * shard_levels(own_key, dims, shards, -0.22, 0.18)
    return jnp.clip(values, -bound, bound).astype(kind)


def gaussian_with(stream_key, shape, spread, most, cuts, heavy, held_as=jnp.bfloat16):
    drawn = spread * jax.random.normal(stream_key, shape, jnp.float32)
    if cuts:
        drawn = drawn * shard_levels(stream_key, shape, cuts, -0.22, 0.18)
    return jnp.clip(strengthened(drawn, jax.random.fold_in(stream_key, 3), *heavy), -most, most).astype(held_as)


def setup_inputs(seed: int = 0) -> dict:
    seeds = jax.random.split(jax.random.key(seed), 5)
    grads = gaussian_with(seeds[0], (TOKENS, K), 1.0, 6.0, ((0, 32),), (0, 1, 32, 2.75))
    covariance = draw_covariance(jax.random.fold_in(seeds[4], 71), 0)
    test_grads = scatter_about(seeds[2], (M, K), K ** -0.5, 0.09375, ((1, 32),))
    inverse_factor = scatter_about(seeds[3], (K, K), K ** -0.5, 0.09375, ((0, 32),))
    return {"grads": grads, "covariance": covariance, "test_grads": test_grads, "inverse_factor": inverse_factor}


def reference(grads, covariance, test_grads, inverse_factor):
    term = jnp.dot(grads.T, grads, preferred_element_type=jnp.float32)
    covariance_out = 0.9 * covariance + term / TOKENS
    preconditioned = jnp.dot(test_grads, inverse_factor, preferred_element_type=jnp.float32).astype(jnp.bfloat16)
    scores = jnp.dot(grads, preconditioned.T, preferred_element_type=jnp.float32)
    return scores, covariance_out
```

```python
import jax
import jax.numpy as jnp
from jax import lax
from jax.sharding import PartitionSpec as P

F32 = jnp.float32
BF16 = jnp.bfloat16


def general(grads, covariance, test_grads, inverse_factor):
    all_features = lax.all_gather(grads, "feat", axis=1, tiled=True)
    examples = grads.shape[0] * lax.axis_size("dp")
    tested = lax.dot_general(
        inverse_factor, test_grads, (((0,), (1,)), ((), ())), preferred_element_type=F32
    )
    term = lax.dot_general(
        all_features, grads, (((0,), (0,)), ((), ())), preferred_element_type=F32
    )
    joined = lax.psum_scatter(
        jnp.concatenate([term, tested], axis=1), "dp", scatter_dimension=0, tiled=True
    )
    width = grads.shape[1]
    owned_pre = joined[:, width:].astype(BF16)
    pre_columns = lax.all_gather(owned_pre, "dp", axis=0, tiled=True)
    scores = jnp.dot(all_features, pre_columns, preferred_element_type=F32)
    return scores, 0.9 * covariance + joined[:, :width] / examples


def send(a, hops):
    return lax.ppermute(a, "dp", hops)


class Chips:
    def __init__(self, n):
        self.n, self.far = n, n // 8
        me = lax.axis_index("dp")
        self.me, self.core = me, me % 2
        self.near = (me // 4 % 2, me // 2 % 2)
        self.z = me // 8

    def flip(self, bit):
        return [(i, i ^ bit) for i in range(self.n)]

    def shift(self, s):
        return [(i, (i + 8 * s) % self.n) for i in range(self.n)]

    def reduce(self, parts, order, link):
        pick = lax.dynamic_index_in_dim
        left = [0, 1]
        for axis in order:
            at = 1 + left.index(axis)
            left.remove(axis)
            here = self.near[axis]
            given = pick(parts, 1 - here, at, keepdims=False).astype(link)
            got = send(given, self.flip(4 >> axis))
            parts = pick(parts, here, at, keepdims=False) + got.astype(F32)
        total = pick(parts, self.z, 0, keepdims=False)
        for s in range(1, self.far):
            given = pick(parts, (self.z + s) % self.far, 0, keepdims=False).astype(link)
            total = total + send(given, self.shift(s)).astype(F32)
        return total

    def join(self, a, here, bit):
        got = send(a, self.flip(bit))
        return jnp.where(here == 0, jnp.stack([a, got], -3), jnp.stack([got, a], -3))

    def gather(self, a):
        seen = [send(a, self.shift(s)) for s in range(self.far - 1, 0, -1)] + [a]
        seen = jnp.stack(seen + seen, 0)
        seen = lax.dynamic_slice_in_dim(seen, self.far - 1 - self.z, self.far, 0)
        for here, bit in ((self.near[0], 4), (self.near[1], 2), (self.core, 1)):
            seen = self.join(seen, here, bit)
        return seen.reshape(self.n * a.shape[0], a.shape[1])


def paired(grads, covariance, test_grads, inverse_factor):
    n = lax.axis_size("dp")
    chips, reach = n // 2, n // 2 + 1
    rows, k = grads.shape
    w = k // n
    at = Chips(n)
    me, core, swap = at.me, at.core, at.flip(1)
    grid = (at.far, 2, 2)

    split = inverse_factor.reshape(-1, chips, 2, w)
    kept = lax.dynamic_index_in_dim(split, core, 2, keepdims=False)
    given = lax.dynamic_index_in_dim(split, 1 - core, 2, keepdims=False)
    other = send(grads, swap)
    factor = jnp.concatenate([kept, send(given, swap)], axis=0).reshape(-1, chips * w)
    tests = jnp.concatenate([test_grads, send(test_grads, swap)], axis=1)
    tested = lax.dot_general(factor, tests, (((0,), (1,)), ((), ())), preferred_element_type=F32)
    tested = tested.reshape(grid + (w, -1))
    half = tested.shape[-1] // 2
    owned_pre = jnp.concatenate(
        [at.reduce(tested[..., :half], (1, 0), F32), at.reduce(tested[..., half:], (0, 1), F32)], axis=1
    ).astype(BF16)
    pre_columns = at.gather(owned_pre)
    scores = jnp.dot(grads, pre_columns, preferred_element_type=F32)

    both = jnp.concatenate([grads, other], axis=0)
    wide = jnp.concatenate([both, both[:, : k // 2]], axis=1)
    shifted = lax.dynamic_slice(wide, (0, core * w), (2 * rows, k + k // 2 - w))

    def strips(first, last):
        return jnp.stack(
            [
                lax.dot_general(
                    shifted[:, 2 * w * q : 2 * w * q + w],
                    shifted[:, 2 * w * q + first * w : 2 * w * q + last * w],
                    (((0,), (0,)), ((), ())),
                    preferred_element_type=F32,
                )
                for q in range(chips)
            ]
        ).reshape(grid + (w, -1))

    cut = reach // 2
    strip = jnp.concatenate(
        [at.reduce(strips(0, cut), (1, 0), BF16), at.reduce(strips(cut, reach), (0, 1), BF16)], axis=1
    )
    blocks = strip.reshape(w, reach, w).transpose(1, 0, 2)
    blocks = jnp.concatenate([blocks, jnp.zeros((n - reach, w, w), F32)], axis=0)

    def turned(a):
        return lax.dynamic_slice_in_dim(jnp.concatenate([a, a], axis=0), (n - me) % n, n, 0)

    mine = turned(blocks)
    mirrored = lax.all_to_all(
        turned(blocks.transpose(0, 2, 1).astype(BF16)), "dp", split_axis=0, concat_axis=0, tiled=True
    )
    ahead = (jnp.arange(n) - me) % n < reach
    term = jnp.where(ahead[:, None, None], mine, mirrored.astype(F32)).transpose(1, 0, 2).reshape(w, k)
    return scores, 0.9 * covariance + term / (rows * n)


def solution(mesh):
    placed = (P("dp", "feat"), P("dp", "feat"), P("feat", "dp"), P("dp", None))
    pairs = mesh.shape["feat"] == 1 and mesh.shape["dp"] % 8 == 0
    return jax.shard_map(
        paired if pairs else general,
        mesh=mesh,
        in_specs=placed,
        out_specs=(P("dp", "feat"), P("dp", "feat")),
        check_vma=False,
    )
```
